256 devices in a mesh: dp: 8 (over y, core), tensor: 32 (over z, x).
Axes of the slice: x: 4, y: 4, z: 8, core: 2. Of those that a mesh axis runs over, the one named last changes fastest.
Arguments:
- hidden: bfloat16 [1280, 16384], P(None, ('dp', 'tensor')), may hold values from -100 to 100
- gain: bfloat16 [1, 16384], P(None, ('dp', 'tensor')), may hold values from 0.5 to 2, as said below
- head_weight: bfloat16 [16384, 65536], P('dp', 'tensor'), may hold values from -3 to 3
- draft_probs: float32 [1280, 65536], P(('dp', 'tensor')), may hold values from 0 to 1, as said below
- draft_ids: int32 [1280], P('dp'), may hold values from 0 to 65535
- reject_at: int32 [256], P('dp'), may hold values from 0 to 4
Outputs:
- token_logprob: float32 [1280], P('dp')
- residual: float32 [256, 65536], P('dp', 'tensor')
The draws below stay inside these ranges and needn't reach their ends.
Inputs may be any that keep to these rules, and one draw needn't show every extreme that they name: `draft_probs`: every row is a probability distribution over the 65536 entries that sums to one. `gain`: positive.
All inputs are finite; a program needn't handle non-finite values.
Results may differ from the reference program's by a relative error of at most 0.0005.
The reference program's roundings to bfloat16 on the way (of `normed`) count: a program that leaves them out, or rounds other values in their place, can miss the bound.
Values may be sent and summed in bfloat16 or wider, within the bound.
A program may use at most 128 MiB of HBM per device.

```python
import jax
import jax.numpy as jnp
from jax import lax

D = 16384
VOCAB = 65536
POS = 5
ROWS = 256
TOKENS = 1280
N_DP = 8


def shared_direction(key, which):
    inner = jax.random.fold_in(key, 501 + which)
    flips = jax.random.bernoulli(inner, 0.5, (D,))
    return jnp.where(flips, 1.0, -1.0).astype(jnp.float32)


def draw_hidden(key, part):
    first, second = jax.random.split(jax.random.fold_in(key, 11), 2)
    ramp = jnp.exp(jnp.log(3.0) * jnp.arange(D, dtype=jnp.float32) / D)
    rough = jax.random.uniform(second, (D,), jnp.float32, 0.5, 1.5)
    base = jnp.clip(jax.random.normal(first, (TOKENS, D), jnp.float32), -5.0, 5.0)
    drawn = base * ramp * rough
    noise = jax.random.uniform(jax.random.fold_in(key, 13), (TOKENS, D), jnp.float32, -0.05, 0.05)
    slot = jnp.arange(TOKENS) % 16
    along_first = shared_direction(key, 0)[None, :] + noise
    along_second = shared_direction(key, 1)[None, :] + noise
    mixed = jnp.where((slot == 3)[:, None], along_first, drawn)
    mixed = jnp.where((slot == 11)[:, None], along_second, mixed)
    return mixed.astype(jnp.bfloat16)


def draw_gain(key, part):
    inner = jax.random.fold_in(key, 23)
    return jnp.clip(1.0 + 0.1 * jax.random.normal(inner, (1, D), jnp.float32), 0.5, 1.5).astype(jnp.bfloat16)


def draw_head_weight(key, part):
    inner = jax.random.fold_in(key, 29)
    base = jnp.clip(jax.random.normal(inner, (D, VOCAB), jnp.float32), -5.0, 5.0) * (9.0 / D) ** 0.5
    quarter = VOCAB // 4
    offsets = jax.random.randint(jax.random.fold_in(key, 601), (4,), 0, quarter)
    places = jnp.arange(4, dtype=jnp.int32) * quarter + offsets
    first = shared_direction(key, 0)
    second = shared_direction(key, 1)
    added = jnp.stack([120.0 * first, 118.0 * first, 230.0 * second, 228.0 * second], axis=1) / D
    return base.at[:, places].add(added).astype(jnp.bfloat16)


def draw_draft_probs(key, part):
    inner = jax.random.fold_in(key, 37)
    scores = 3.0 * jax.random.normal(inner, (TOKENS, VOCAB), jnp.float32)
    return jax.nn.softmax(scores, axis=1)


def set_ends(values, own_key, least, largest):
    longest = values.shape.index(max(values.shape))
    spots = []
    for shift in (0, 1):
        where = [jax.random.randint(jax.random.fold_in(own_key, axis), (), 0, length) for axis, length in enumerate(values.shape)]
        where[longest] = (where[longest] + shift) % values.shape[longest]
        spots.append(tuple(where))
    return values.at[spots[0]].set(least).at[spots[1]].set(largest)


def setup_inputs(seed: int = 0) -> dict:
    keys = jax.random.split(jax.random.key(seed), 7)
    hidden = draw_hidden(jax.random.fold_in(keys[6], 71), 0)
    gain = draw_gain(jax.random.fold_in(keys[6], 71), 0)
    head_weight = draw_head_weight(jax.random.fold_in(keys[6], 71), 0)
    draft_probs = draw_draft_probs(jax.random.fold_in(keys[6], 71), 0)
    draft_ids = set_ends(jax.random.randint(keys[4], (TOKENS,), 0, VOCAB), jax.random.fold_in(keys[4], 1), 0, VOCAB - 1).astype(jnp.int32)
    reject_at = set_ends(jax.random.randint(keys[5], (ROWS,), 0, POS), jax.random.fold_in(keys[5], 1), 0, POS - 1).astype(jnp.int32)
    return {"hidden": hidden, "gain": gain, "head_weight": head_weight, "draft_probs": draft_probs, "draft_ids": draft_ids, "reject_at": reject_at}


def reference(hidden, gain, head_weight, draft_probs, draft_ids, reject_at):
    values = hidden.astype(jnp.float32)
    squares = lax.optimization_barrier(jnp.sum(values * values, axis=1))
    normed = (values * lax.rsqrt(squares / D + 1e-05)[:, None] * gain.astype(jnp.float32)).astype(jnp.bfloat16)
    block_width = D // N_DP
    logits = jnp.zeros((TOKENS, VOCAB), jnp.float32)
    for block in range(N_DP):
        partial_b = jnp.dot(normed[:, block * block_width:(block + 1) * block_width], head_weight[block * block_width:(block + 1) * block_width], preferred_element_type=jnp.float32)
        logits = logits + partial_b
    top = lax.optimization_barrier(jnp.max(logits, axis=1))
    logz = top + jnp.log(lax.optimization_barrier(jnp.sum(jnp.exp(logits - top[:, None]), axis=1)))
    picked = jnp.take_along_axis(logits, draft_ids.astype(jnp.int32)[:, None], axis=1)[:, 0]
    token_logprob = picked - logz
    where_at = reject_at.astype(jnp.int32)
    grid = logits.reshape(ROWS, POS, VOCAB)
    chosen = jnp.take_along_axis(grid, where_at[:, None, None], axis=1)[:, 0]
    chosen_logz = jnp.take_along_axis(logz.reshape(ROWS, POS), where_at[:, None], axis=1)[:, 0]
    drafts = jnp.take_along_axis(draft_probs.reshape(ROWS, POS, VOCAB), where_at[:, None, None], axis=1)[:, 0]
    target = jnp.exp(chosen - chosen_logz[:, None])
    kept = jnp.maximum(target - drafts, 0.0)
    mass = lax.optimization_barrier(jnp.sum(kept, axis=1))
    residual = VOCAB * kept / mass[:, None]
    return (token_logprob, residual)
```

```python
import jax
import jax.numpy as jnp
from jax import lax
from jax.experimental import pallas as pl
from jax.experimental.pallas import tpu as pltpu
from jax.sharding import Mesh
from jax.sharding import PartitionSpec as P

D = 16384
VOCAB = 65536
POS = 5
EPS = 1e-05
NY, NC, NZ, NX = 4, 2, 8, 4
OWNERS = NY * NC
CHUNKS = 5
TOKENS = 1280
CT = TOKENS // CHUNKS
PIECE = CT // OWNERS
FEAT = 64
BLOCK = FEAT * NZ * NX
WIDTH = VOCAB // (NZ * NX)
HALF = WIDTH // 2
ROWS = TOKENS // OWNERS
KINDS = ("z", "x", "z", "x", "z")
MESH = pl.DeviceIdType.MESH
TENSOR = ("z", "x")
DP = ("y", "core")
F32 = jnp.float32
BF16 = jnp.bfloat16


def wrapped(i, n):
    return lax.rem(i + n, n)


def send(src, dst, send_sem, recv_sem, device):
    pltpu.make_async_remote_copy(
        src_ref=src, dst_ref=dst, send_sem=send_sem, recv_sem=recv_sem, device_id=device, device_id_type=MESH
    ).start()


def got(ref, sem):
    pltpu.make_async_copy(ref, ref, sem).wait()


def head_kernel(
    hid_hbm, gain_ref, w_hbm, out_ref,
    hid, g, w, xt, part, pair, r1p, r1m, r2p, r2m, gcol, rs,
    sx_out, sx_in, sz_in, sc_out, sc_in, sy_in,
    local_sem, g_send, g_recv, r_send, r_recv, s_send, s_recv,
):
    y, core = lax.axis_index("y"), lax.axis_index("core")
    z, x = lax.axis_index("z"), lax.axis_index("x")
    d = 1 - 2 * core
    zf, zb = wrapped(z + d, NZ), wrapped(z - d, NZ)
    xf, xb = wrapped(x + d, NX), wrapped(x - d, NX)
    yp, ym = wrapped(y + 1, NY), wrapped(y - 1, NY)
    other = 1 - core

    hid_in = pltpu.make_async_copy(hid_hbm, hid, local_sem.at[0])
    hid_in.start()
    w_in = pltpu.make_async_copy(w_hbm, w, local_sem.at[1])
    w_in.start()

    barrier = pltpu.get_barrier_semaphore()
    for k in range(1, NZ):
        pl.semaphore_signal(barrier, inc=1, device_id={"z": wrapped(z + k, NZ)}, device_id_type=MESH)
    for k in range(1, NX):
        pl.semaphore_signal(barrier, inc=1, device_id={"x": wrapped(x + k, NX)}, device_id_type=MESH)
    for k in range(1, NY):
        pl.semaphore_signal(barrier, inc=1, device_id={"y": wrapped(y + k, NY)}, device_id_type=MESH)
    pl.semaphore_signal(barrier, inc=1, device_id={"core": other}, device_id_type=MESH)

    def block(c, zz, xx):
        return g.at[c, pl.ds(pl.multiple_of((zz * NX + xx) * FEAT, FEAT), FEAT), :]

    def line(c, zz):
        return g.at[c, pl.ds(pl.multiple_of(zz * (NX * FEAT), NX * FEAT), NX * FEAT), :]

    def zat(k):
        return wrapped(z + d * k, NZ)

    hid_in.wait()
    lanes = lax.broadcasted_iota(jnp.int32, (FEAT, 128), 1) // PIECE
    mine = pl.ds(pl.multiple_of((z * NX + x) * FEAT, FEAT), FEAT)
    sx_out[...] = jnp.zeros_like(sx_out)
    for c in range(CHUNKS):
        for h in range(2):
            tile = jnp.zeros((FEAT, 128), F32)
            for j in range(4):
                place = h * 4 + j
                owner = (place % NY) * NC + place // NY
                start = owner * ROWS + PIECE * c
                at, off = start // 128, start % 128
                source = hid[:, at * 128 : at * 128 + 128].astype(F32)
                shift = (PIECE * j - off) % 128
                moved = pltpu.roll(source, shift, 1) if shift else source
                tile = jnp.where(lanes == j, moved, tile)
            g[c, mine, h * 128 : h * 128 + 128] = tile.astype(BF16)
            sx_out[2 * c + h : 2 * c + h + 1, :] = jnp.sum(tile * tile, axis=0, keepdims=True)
    both = jnp.concatenate([gain_ref[...].astype(F32)] * 2, axis=1)
    lane = lax.broadcasted_iota(jnp.int32, (1, 128), 1) // FEAT
    sx_out[10:11, :] = jnp.where(lane == lax.rem(x, 2), both, 0.0)

    pl.semaphore_wait(barrier, NZ + NX + NY - 3 + 1)

    def z_first(c):
        def pass_on(k, zz, device):
            ref = block(c, zz, x)
            send(ref, ref, g_send.at[c], g_recv.at[c, k], {"z": device})

        def arrived(k, zz):
            got(block(c, zz, x), g_recv.at[c, k])

        def across(ks, xx, device, k):
            for kk in ks:
                ref = block(c, zat(kk), xx)
                send(ref, ref, g_send.at[c], g_recv.at[c, k], {"x": device})

        def group(count, k):
            got(g.at[c, pl.ds(0, count * FEAT), :], g_recv.at[c, k])

        near, far = (0, -1, 1, -2, 2), (-3, 3, -4)

        def s0():
            pass_on(0, z, zf)
            pass_on(4, z, zb)

        def s1():
            arrived(0, zat(-1))
            pass_on(1, zat(-1), zf)
            arrived(4, zat(1))
            pass_on(5, zat(1), zb)

        def s2():
            arrived(1, zat(-2))
            pass_on(2, zat(-2), zf)
            arrived(5, zat(2))
            pass_on(6, zat(2), zb)
            across(near, x, xf, 7)
            across(near, x, xb, 8)

        def s3():
            arrived(2, zat(-3))
            pass_on(3, zat(-3), zf)
            arrived(6, zat(3))

        def s4():
            arrived(3, zat(-4))
            across(far, x, xf, 9)
            across(far, x, xb, 10)
            group(5, 7)
            across(near, xb, xf, 11)
            group(5, 8)

        def s5():
            group(3, 9)
            group(3, 10)
            across(far, xf, xb, 12)

        def s6():
            group(5, 11)
            group(3, 12)

        return [s0, s1, s2, s3, s4, s5, s6]

    def x_first(c):
        def pass_on(k, zz, device):
            ref = line(c, zz)
            send(ref, ref, g_send.at[c], g_recv.at[c, k], {"z": device})

        def arrived(k, zz):
            got(line(c, zz), g_recv.at[c, k])

        def s0():
            for k in range(1, NX):
                ref = block(c, z, x)
                send(ref, ref, g_send.at[c], g_recv.at[c, 6 + k], {"x": wrapped(x + k, NX)})

        def s1():
            for k in range(1, NX):
                got(block(c, z, wrapped(x - k, NX)), g_recv.at[c, 6 + k])
            pass_on(0, z, zf)
            pass_on(4, z, zb)

        def s2():
            arrived(0, zat(-1))
            pass_on(1, zat(-1), zf)
            arrived(4, zat(1))
            pass_on(5, zat(1), zb)

        def s3():
            arrived(1, zat(-2))
            pass_on(2, zat(-2), zf)
            arrived(5, zat(2))
            pass_on(6, zat(2), zb)

        def s4():
            arrived(2, zat(-3))
            pass_on(3, zat(-3), zf)
            arrived(6, zat(3))

        def s5():
            arrived(3, zat(-4))

        return [s0, s1, s2, s3, s4, s5]

    def q0():
        for k in range(1, NX):
            send(sx_out, sx_in.at[k - 1], s_send.at[0], s_recv.at[k - 1], {"x": wrapped(x + k, NX)})

    def q1():
        for k in range(1, NX):
            got(sx_in.at[k - 1], s_recv.at[k - 1])
        total = sx_out[0:10, :] + sx_in[0, 0:10, :] + sx_in[1, 0:10, :] + sx_in[2, 0:10, :]
        sz_in[z, 0:10, :] = total
        own = sx_out[10:11, :]
        one, two, three = sx_in[0, 10:11, :], sx_in[1, 10:11, :], sx_in[2, 10:11, :]
        odd = lax.rem(x, 2) == 1
        with_next = jnp.where(odd, one, three)
        first = jnp.where(odd, three, one)
        mate = own + with_next
        rest = two + first
        low = x < 2
        sz_in[z, 10:11, :] = jnp.where(low, mate, rest)
        sz_in[z, 11:12, :] = jnp.where(low, rest, mate)
        for k in range(1, NZ):
            send(sz_in.at[z], sz_in.at[z], s_send.at[1], s_recv.at[2 + k], {"z": wrapped(z + k, NZ)})

    def q2():
        for k in range(1, NZ):
            got(sz_in.at[wrapped(z - k, NZ)], s_recv.at[2 + k])
        total = sz_in[0, 0:10, :]
        for k in range(1, NZ):
            total = total + sz_in[k, 0:10, :]
        sc_out[0:10, :] = total
        send(sc_out, sc_in, s_send.at[2], s_recv.at[10], {"core": other})
        for k in range(NZ):
            for half in range(2):
                row = jnp.broadcast_to(sz_in[k, 10 + half : 11 + half, :], (128, 128))
                gcol[pl.ds((2 * k + half) * 128, 128), :] = row.T

    def q3():
        got(sc_in, s_recv.at[10])
        sy_in[y, 0:10, :] = sc_out[0:10, :] + sc_in[0:10, :]
        for k in range(1, NY):
            send(sy_in.at[y], sy_in.at[y], s_send.at[3], s_recv.at[10 + k], {"y": wrapped(y + k, NY)})

    def q4():
        for k in range(1, NY):
            got(sy_in.at[wrapped(y - k, NY)], s_recv.at[10 + k])
        total = (sy_in[0, 0:10, :] + sy_in[1, 0:10, :]) + (sy_in[2, 0:10, :] + sy_in[3, 0:10, :])
        rs[0:10, :] = lax.rsqrt(total / D + EPS)

    def compute(c):
        scale = [jnp.broadcast_to(rs[2 * c + h : 2 * c + h + 1, :], (128, 128)) for h in range(2)]

        @pl.loop(0, BLOCK // 128)
        def _(k):
            rows = pl.ds(pl.multiple_of(k * 128, 128), 128)
            gains = gcol[rows, :]
            for h in range(2):
                values = g[c, rows, h * 128 : h * 128 + 128].astype(F32)
                normed = (values * scale[h] * gains).astype(BF16)
                xt[h * 128 : h * 128 + 128, rows] = normed.T

        if c == 0:
            w_in.wait()

        @pl.loop(0, WIDTH // 256)
        def _(k):
            columns = pl.ds(pl.multiple_of(k * 256, 256), 256)
            part[c, :, columns] = jnp.dot(xt[...], w[:, columns], preferred_element_type=F32)

        theirs = pl.ds(pl.multiple_of(other * 128, 128), 128)
        send(part.at[c, theirs, :], pair.at[c], r_send.at[c], r_recv.at[c, 0], {"core": other})

    def own_rows(yy):
        return pl.ds(pl.multiple_of(core * 128 + yy * PIECE, PIECE), PIECE)

    low, high = pl.ds(0, HALF), pl.ds(HALF, HALF)

    def reduce_a(c):
        got(pair.at[c], r_recv.at[c, 0])

        def add(yy):
            rows = own_rows(yy)
            part[c, rows, :] = part[c, rows, :] + pair[c, pl.ds(pl.multiple_of(yy * PIECE, PIECE), PIECE), :]

        across = wrapped(y + 2, NY)
        add(across)
        send(part.at[c, own_rows(across), low], r1p.at[c], r_send.at[c], r_recv.at[c, 1], {"y": yp})
        send(part.at[c, own_rows(across), high], r1m.at[c], r_send.at[c], r_recv.at[c, 2], {"y": ym})
        add(yp)
        send(part.at[c, own_rows(yp), high], r2p.at[c, :, high], r_send.at[c], r_recv.at[c, 3], {"y": yp})
        add(ym)
        send(part.at[c, own_rows(ym), low], r2m.at[c, :, low], r_send.at[c], r_recv.at[c, 4], {"y": ym})
        add(y)

    def reduce_b(c):
        got(r1p.at[c], r_recv.at[c, 1])
        rows = own_rows(yp)
        part[c, rows, 0:HALF] = part[c, rows, 0:HALF] + r1p[c]
        send(part.at[c, rows, low], r2p.at[c, :, low], r_send.at[c], r_recv.at[c, 5], {"y": yp})
        got(r1m.at[c], r_recv.at[c, 2])
        rows = own_rows(ym)
        part[c, rows, HALF:WIDTH] = part[c, rows, HALF:WIDTH] + r1m[c]
        send(part.at[c, rows, high], r2m.at[c, :, high], r_send.at[c], r_recv.at[c, 6], {"y": ym})

    def reduce_c(c):
        got(r2p.at[c, :, high], r_recv.at[c, 3])
        got(r2m.at[c, :, low], r_recv.at[c, 4])
        got(r2p.at[c, :, low], r_recv.at[c, 5])
        got(r2m.at[c, :, high], r_recv.at[c, 6])
        out_ref[c * PIECE : (c + 1) * PIECE, :] = part[c, own_rows(y), :] + (r2p[c] + r2m[c])

    steps = {"z": z_first, "x": x_first}
    gather = [steps[kind](c) for c, kind in enumerate(KINDS)]
    squares = [q0, q1, q2, q3, q4]
    done = 0
    pending_a, pending_b = [], []
    rounds = max(2 * c + len(gather[c]) for c in range(CHUNKS))
    for r in range(rounds):
        for c in range(CHUNKS):
            if 0 <= r - 2 * c < len(gather[c]):
                gather[c][r - 2 * c]()
        if r < len(squares):
            squares[r]()
        while pending_b and pending_b[0][1] <= r:
            reduce_b(pending_b.pop(0)[0])
        while pending_a and pending_a[0][1] <= r:
            c = pending_a.pop(0)[0]
            reduce_a(c)
            pending_b.append((c, r + 2))
        while done < CHUNKS and 2 * done + len(gather[done]) - 1 <= r:
            compute(done)
            pending_a.append((done, r + 1))
            done += 1
    for c, _ in list(pending_b):
        reduce_b(c)
    pending_b = []
    for c, _ in pending_a:
        reduce_a(c)
        pending_b.append((c, 0))
    for c, _ in pending_b:
        reduce_b(c)
    for c in range(CHUNKS):
        reduce_c(c)

    for c in range(CHUNKS):
        got(g.at[c, pl.ds(0, 31 * FEAT), :], g_send.at[c])
        got(part.at[c, pl.ds(0, 224), :], r_send.at[c])
    got(sx_in, s_send.at[0])
    got(sz_in.at[pl.ds(0, NZ - 1)], s_send.at[1])
    got(sc_in, s_send.at[2])
    got(sy_in.at[pl.ds(0, NY - 1)], s_send.at[3])


def owned_logits(hidden, gain, head_weight):
    vmem = pltpu.VMEM
    dma = pltpu.SemaphoreType.DMA
    return pl.pallas_call(
        head_kernel,
        out_shape=jax.ShapeDtypeStruct((ROWS, WIDTH), F32),
        in_specs=[
            pl.BlockSpec(memory_space=pl.ANY),
            pl.BlockSpec(memory_space=pltpu.VMEM),
            pl.BlockSpec(memory_space=pl.ANY),
        ],
        out_specs=pl.BlockSpec(memory_space=pltpu.VMEM),
        scratch_shapes=[
            vmem((FEAT, TOKENS), BF16),
            vmem((CHUNKS, BLOCK, CT), BF16),
            vmem((BLOCK, WIDTH), BF16),
            vmem((CT, BLOCK), BF16),
            vmem((CHUNKS, CT, WIDTH), F32),
            vmem((CHUNKS, CT // 2, WIDTH), F32),
            vmem((CHUNKS, PIECE, HALF), F32),
            vmem((CHUNKS, PIECE, HALF), F32),
            vmem((CHUNKS, PIECE, WIDTH), F32),
            vmem((CHUNKS, PIECE, WIDTH), F32),
            vmem((BLOCK, 128), F32),
            vmem((16, 128), F32),
            vmem((16, 128), F32),
            vmem((NX - 1, 16, 128), F32),
            vmem((NZ, 16, 128), F32),
            vmem((16, 128), F32),
            vmem((16, 128), F32),
            vmem((NY, 16, 128), F32),
            dma((2,)),
            dma((CHUNKS,)),
            dma((CHUNKS, 13)),
            dma((CHUNKS,)),
            dma((CHUNKS, 7)),
            dma((4,)),
            dma((14,)),
        ],
        compiler_params=pltpu.CompilerParams(
            collective_id=0, has_side_effects=True, vmem_limit_bytes=60 * 1024 * 1024
        ),
        name="head",
    )(hidden.T, gain, head_weight)


def sent_to_all(shard, axis):
    devices = lax.axis_size(axis)
    return lax.all_to_all(
        jnp.broadcast_to(shard[None], (devices, *shard.shape)), axis, 0, 0, tiled=True
    )


def exchanged(local_rows):
    out = local_rows.reshape(NZ, NX, 1, WIDTH)
    out = lax.all_to_all(out, "z", 0, 0, tiled=True)
    out = lax.all_to_all(out, "x", 1, 1, tiled=True)
    return out.reshape(NZ * NX, WIDTH)


def shards(hidden, gain, head_weight, draft_probs, draft_ids, reject_at):
    owned = draft_probs.shape[0] // POS
    mine = lax.dynamic_slice_in_dim(reject_at, lax.axis_index(TENSOR) * owned, owned, 0)
    local_rows = jnp.take_along_axis(
        draft_probs.reshape(owned, POS, draft_probs.shape[1]), mine[:, None, None], axis=1
    )[:, 0]
    drafts = exchanged(local_rows)
    logits = owned_logits(hidden, gain, head_weight)
    width = logits.shape[1]
    columns = lax.broadcasted_iota(jnp.int32, (1, width), 1) + lax.axis_index(TENSOR) * width
    local_max = jnp.max(logits, axis=1)
    local_pick = jnp.sum(jnp.where(columns == draft_ids[:, None], logits, 0.0), axis=1)
    local_total = jnp.sum(jnp.exp(logits - local_max[:, None]), axis=1)
    stats = sent_to_all(jnp.stack([local_max, local_total, local_pick]), TENSOR)
    tops, totals, picks = stats[:, 0], stats[:, 1], stats[:, 2]
    top = jnp.max(tops, axis=0)
    total = jnp.sum(totals * jnp.exp(tops - top), axis=0)
    picked = jnp.sum(picks, axis=0)
    logz = top + jnp.log(total)
    token_logprob = picked - logz
    requests = reject_at.shape[0]
    hot = lax.broadcasted_iota(jnp.int32, (requests, POS), 1) == reject_at[:, None]
    chosen = jnp.sum(jnp.where(hot[:, :, None], logits.reshape(requests, POS, width), 0.0), axis=1)
    chosen_logz = jnp.sum(jnp.where(hot, logz.reshape(requests, POS), 0.0), axis=1)
    target = jnp.exp(chosen - chosen_logz[:, None])
    kept = jnp.maximum(target - drafts, 0.0)
    mass = jnp.sum(sent_to_all(jnp.sum(kept, axis=1), TENSOR), axis=0)
    residual = VOCAB * kept / mass[:, None]
    return (token_logprob, residual)


def solution(mesh):
    finer = Mesh(mesh.devices.reshape(NY, NC, NZ, NX), ("y", "core", "z", "x"))
    return jax.shard_map(
        shards,
        mesh=finer,
        in_specs=(
            P(None, (*DP, *TENSOR)),
            P(None, (*DP, *TENSOR)),
            P(DP, TENSOR),
            P((*DP, *TENSOR), None),
            P(DP),
            P(DP),
        ),
        out_specs=(P(DP), P(DP, TENSOR)),
        check_vma=False,
    )
```
